32 devices in a mesh: seq: 8 (over z, y), head: 4 (over x, core).
Axes of the slice: x: 2, y: 2, z: 4, core: 2. Of those that a mesh axis runs over, the one named last changes fastest.
Arguments:
- hidden_states: bfloat16 [8, 512, 3584], P(None, 'seq', 'head'), may hold values from -6 to 6
- boundary: int32 [8, 64], replicated, may hold values from 0 to 511, as said below
- valid: int32 [8, 64], replicated, may hold values from 0 to 1, as said below
- pairs: int32 [8, 2], replicated, may hold values from 0 to 7, as said below
- w_first: bfloat16 [3584, 4096], P('seq', 'head'), may hold values from -0.09375 to 0.09375
- b_first: float32 [4096], P('head'), may hold values from -3 to 3
- w_second: float32 [4096], P('head'), may hold values from -0.09375 to 0.09375
Outputs:
- step_reward: float32 [8, 64], replicated
- trace_score: float32 [8], replicated
- margin: float32 [8], replicated
The draws below stay inside these ranges and needn't reach their ends.
Inputs may be any that keep to these rules, and one draw needn't show every extreme that they name: Within a trace the 64 boundary positions are distinct and increasing. In each trace the ones come first; every trace has 16 to 64 valid steps. `pairs`: the two traces of a pair differ.
All inputs are finite; a program needn't handle non-finite values.
Results may differ from the reference program's by a relative error of at most 0.0003.
Values may be sent and summed in bfloat16 or wider, within the bound.
A program may use at most 64 MiB of HBM per device.

```python
import jax
import jax.numpy as jnp

D = 3584
HID = 4096
STEPS = 64
TRACES = 8
SEQLEN = 512
PAIRS = 8


def count_steps(key):
    return jax.random.randint(jax.random.fold_in(key, 11), (TRACES,), 16, STEPS + 1)


def draw_boundary(key, part):
    keys = jax.random.split(jax.random.fold_in(key, 23), TRACES)

    def one_trace(single):
        chosen = jax.random.permutation(single, SEQLEN)[:STEPS]
        return jnp.sort(chosen)
    return jax.vmap(one_trace)(keys).astype(jnp.int32)


def draw_valid(key, part):
    counts = count_steps(key)
    slots = jnp.arange(STEPS)[None, :]
    return (slots < counts[:, None]).astype(jnp.int32)


def draw_pairs(key, part):
    first = jax.random.randint(jax.random.fold_in(key, 31), (PAIRS,), 0, TRACES)
    offset = jax.random.randint(jax.random.fold_in(key, 37), (PAIRS,), 1, TRACES)
    second = (first + offset) % TRACES
    return jnp.stack([first, second], axis=1).astype(jnp.int32)


def block_scale(rng, dims, shards, smallest, top_value):
    def one(position, parts):
        draws = jax.random.uniform(jax.random.fold_in(jax.random.fold_in(rng, 6), position), (parts,), jnp.float32, smallest / len(shards), top_value / len(shards))
        return jnp.repeat(jnp.exp(draws), dims[position] // parts).reshape((-1,) + (1,) * (len(dims) - position - 1))

    level = one(*shards[0])
    for cut in shards[1:]:
        level = level * one(*cut)
    return level


def noise(key, extent, spread, most, pieces=(), kind=jnp.bfloat16):
    loudness = block_scale(key, extent, pieces, -0.22, 0.18) if pieces else 1.0
    entries = jax.random.normal(key, extent, jnp.float32) * spread * loudness
    return jnp.minimum(jnp.maximum(entries, -most), most).astype(kind)


def setup_inputs(seed: int = 0) -> dict:
    arg_keys = jax.random.split(jax.random.key(seed), 8)
    hidden_states = noise(arg_keys[0], (TRACES, SEQLEN, D), 1.0, 6.0, ((1, 8), (2, 4)))
    boundary = draw_boundary(jax.random.fold_in(arg_keys[7], 71), 0)
    valid = draw_valid(jax.random.fold_in(arg_keys[7], 71), 0)
    pairs = draw_pairs(jax.random.fold_in(arg_keys[7], 71), 0)
    w_first = noise(arg_keys[4], (D, HID), D ** -0.5, 0.09375, ((0, 8), (1, 4)))
    b_first = noise(arg_keys[5], (HID,), 0.5, 3.0, ((0, 4),), jnp.float32)
    w_second = noise(arg_keys[6], (HID,), HID ** -0.5, 0.09375, ((0, 4),), jnp.float32)
    return dict(hidden_states=hidden_states, boundary=boundary, valid=valid, pairs=pairs, w_first=w_first, b_first=b_first, w_second=w_second)


def reference(hidden_states, boundary, valid, pairs, w_first, b_first, w_second):
    picked = jnp.take_along_axis(hidden_states, boundary[:, :, None].astype(jnp.int32), axis=1)
    rows = picked.reshape(TRACES * STEPS, D)
    pre = jnp.dot(rows, w_first, preferred_element_type=jnp.float32) + b_first
    logit = jnp.sum(jnp.maximum(pre, 0.0) * w_second, axis=-1).reshape(TRACES, STEPS)
    live = valid == 1
    step_reward = jnp.where(live, logit, jnp.float32(0.0))
    trace_score = jnp.min(jnp.where(live, logit, jnp.float32(1e30)), axis=1)
    margin = trace_score[pairs[:, 0]] - trace_score[pairs[:, 1]]
    return step_reward, trace_score, margin
```

```python
import functools

import jax
import jax.numpy as jnp
from jax import lax
from jax.experimental import pallas as pl
from jax.experimental.pallas import tpu as pltpu
from jax.sharding import PartitionSpec as P

MESH = pl.DeviceIdType.MESH


def score_rows(rows, w_first, b_first, w_second):
    pre = jnp.dot(
        rows, lax.all_gather(w_first, "seq", axis=0, tiled=True), preferred_element_type=jnp.float32
    )
    return jnp.sum(jnp.maximum(pre + b_first, 0.0) * w_second, axis=-1)


def per_device(hidden_states, boundary, valid, pairs, w_first, b_first, w_second):
    traces, tok_dev, quarter = hidden_states.shape
    offset = lax.axis_index("seq") * tok_dev
    positions = offset + jnp.arange(tok_dev, dtype=jnp.int32)
    hits = boundary[:, :, None] == positions[None, None, :]
    whole = lax.all_gather(hidden_states, "head", axis=2, tiled=True)
    token_logit = score_rows(
        whole.reshape(traces * tok_dev, whole.shape[2]), w_first, b_first, w_second
    )
    token_logit = token_logit.reshape(traces, tok_dev)
    partial_logit = jnp.sum(jnp.where(hits, token_logit[:, None, :], 0.0), axis=2)
    logit = lax.psum(partial_logit, ("seq", "head"))
    live = valid == 1
    step_reward = jnp.where(live, logit, jnp.float32(0.0))
    trace_score = jnp.min(jnp.where(live, logit, jnp.float32(1e30)), axis=1)
    trace_ids = jnp.arange(traces, dtype=jnp.int32)[None, :]
    winner = jnp.sum(jnp.where(pairs[:, 0:1] == trace_ids, trace_score[None, :], 0.0), axis=1)
    loser = jnp.sum(jnp.where(pairs[:, 1:2] == trace_ids, trace_score[None, :], 0.0), axis=1)
    return (step_reward, trace_score, winner - loser)


def kernel(
    n_seq, n_head, hid, bnd, valid, pairs, w, b, w2, reward, score, margin,
    xout, xin, xacc, xup, xdn, xall, wown, wall, psend, precv, fsend, frecv,
    s_x1, r_x1, s_w, r_w, s_x2, r_up, r_dn, s_x3, r_x3, s_p, r_p, s_f, r_f,
):
    traces, toks, _ = hid.shape
    half = traces // 2
    planes = n_seq // 2
    depth = w.shape[0]
    cols = w.shape[1] // 2
    s = lax.axis_index("seq")
    h = lax.axis_index("head")
    z = s // 2
    y = s % 2
    other = 1 - y

    def remote(src, dst, send, recv, to_s, to_h):
        return pltpu.make_async_remote_copy(
            src_ref=src, dst_ref=dst, send_sem=send, recv_sem=recv,
            device_id=(to_s, to_h), device_id_type=MESH,
        )

    across = s + 1 - 2 * y
    h_core = h + 1 - 2 * (h % 2)
    h_x = lax.rem(h + 2, n_head)

    def pick(t):
        pos = lax.broadcasted_iota(jnp.int32, (toks, bnd.shape[1]), 0) + s * toks
        hot = jnp.where(bnd[pl.ds(t, 1), :] == pos, 1.0, 0.0).astype(jnp.bfloat16)
        got = lax.dot_general(
            hot, hid[t], (((0,), (0,)), ((), ())), preferred_element_type=jnp.float32
        )
        return got.astype(jnp.bfloat16)

    def copy_x1(k):
        return remote(xout.at[k], xin.at[k], s_x1.at[k], r_x1.at[k], across, h)

    for k in range(half):
        xout[k] = pick(other * half + k)
        copy_x1(k).start()

    def my_cols(which):
        return pl.ds(pl.multiple_of(which * cols, cols), cols)

    rows = pl.ds(pl.multiple_of(y * depth, depth), depth)
    wown[...] = w[:, my_cols(other)]
    copy_w = remote(wown, wall.at[rows], s_w, r_w, across, h)
    copy_w.start()
    wall[rows, :] = w[:, my_cols(y)]

    for k in range(half):
        xacc[k] = pick(y * half + k)

    is_root = z == h
    from_up = (z >= h) & (z < planes - 1)
    from_dn = (z <= h) & (z > 0)

    def copy_down(k):
        return remote(xacc.at[k], xup.at[k], s_x2.at[k], r_up.at[k], lax.rem(s + n_seq - 2, n_seq), h)

    def copy_up(k):
        return remote(xacc.at[k], xdn.at[k], s_x2.at[k], r_dn.at[k], lax.rem(s + 2, n_seq), h)

    def chain(k):
        copy_x1(k).wait_recv()
        xacc[k] = xacc[k] + xin[k]

        @pl.when(from_up)
        def _():
            copy_down(k).wait_recv()
            xacc[k] = xacc[k] + xup[k]

        @pl.when(from_dn)
        def _():
            copy_up(k).wait_recv()
            xacc[k] = xacc[k] + xdn[k]

        @pl.when(z > h)
        def _():
            copy_down(k).start()

        @pl.when(z < h)
        def _():
            copy_up(k).start()

        @pl.when(is_root)
        def _():
            xall[y * half + k] = xacc[k]

    same_core = (h % 2) == (z % 2)
    same_x = (h // 2) == (z // 2)

    def copy_x3(t, way):
        to_s, to_h = ((s, h_core), (across, h), (s, h_x))[way]
        return remote(xall.at[t], xall.at[t], s_x3.at[t, way], r_x3.at[t], to_s, to_h)

    def spread(k):
        for y0 in range(2):
            t = y0 * half + k

            @pl.when(jnp.logical_not(is_root & (y == y0)))
            def _():
                copy_x3(t, 0).wait_recv()

            @pl.when(same_core & same_x & (y == y0))
            def _():
                copy_x3(t, 2).start()

            @pl.when(same_core & (y == y0))
            def _():
                copy_x3(t, 1).start()

            @pl.when(same_core)
            def _():
                copy_x3(t, 0).start()

    for k in range(half):
        chain(k)
        if k >= 1:
            spread(k - 1)
    spread(half - 1)

    copy_w.wait_recv()

    def copy_p(t):
        to_s = lax.rem(s + n_seq - 2, n_seq) if t < half else lax.rem(s + 2, n_seq)
        return remote(psend.at[t], precv.at[t], s_p.at[t], r_p.at[t], to_s, h)

    bias = b[:, my_cols(y)]
    out_row = w2[:, my_cols(y)]
    lanes = lax.broadcasted_iota(jnp.int32, (xall.shape[1], 128), 1)
    fsend[...] = jnp.zeros_like(fsend)
    for k in range(half):
        for t in (k, half + k):
            first = planes - 1 if t < half else 0
            last = 0 if t < half else planes - 1
            psend[t] = jnp.dot(xall[t], wall[...], preferred_element_type=jnp.float32)

            @pl.when(z != first)
            def _():
                copy_p(t).wait_recv()
                psend[t] = psend[t] + precv[t]

            @pl.when(z != last)
            def _():
                copy_p(t).start()

            @pl.when(z == last)
            def _():
                act = jnp.maximum(psend[t] + bias, 0.0) * out_row
                part = jnp.sum(act, axis=1, keepdims=True)
                fsend[...] = fsend[...] + jnp.where(lanes == t, part, 0.0)

    is_end = (z == 0) | (z == planes - 1)
    slots = 4 * n_head
    me = s * n_head + h
    n_dev = n_seq * n_head
    slot = jnp.where(z == 0, 0, 1) * (2 * n_head) + y * n_head + h

    def copy_f(d):
        to = lax.rem(me + d, n_dev)
        return remote(
            frecv.at[slot], frecv.at[slot], s_f.at[d], r_f.at[slot], to // n_head, lax.rem(to, n_head)
        )

    @pl.when(is_end)
    def _():
        frecv[slot] = jnp.transpose(fsend[...])[: frecv.shape[1], :]
        for d in range(1, n_dev):
            copy_f(d).start()

    logit = jnp.zeros(frecv.shape[1:], jnp.float32)
    for i in range(slots):

        @pl.when(jnp.logical_not(is_end & (slot == i)))
        def _():
            remote(frecv.at[i], frecv.at[i], s_f.at[0], r_f.at[i], across, h).wait_recv()

        logit = logit + frecv[i]

    live = valid[...] == 1
    reward[...] = jnp.where(live, logit, 0.0)
    low = jnp.min(jnp.where(live, logit, 1e30), axis=1, keepdims=True)
    score[...] = low
    eye = lax.broadcasted_iota(jnp.int32, (traces, traces), 0) == lax.broadcasted_iota(
        jnp.int32, (traces, traces), 1
    )
    row = jnp.sum(jnp.where(eye, low, 0.0), axis=0, keepdims=True)
    ids = lax.broadcasted_iota(jnp.int32, (pairs.shape[0], traces), 1)
    winner = jnp.sum(jnp.where(pairs[:, 0:1] == ids, row, 0.0), axis=1, keepdims=True)
    loser = jnp.sum(jnp.where(pairs[:, 1:2] == ids, row, 0.0), axis=1, keepdims=True)
    margin[...] = winner - loser

    copy_w.wait_send()
    for k in range(half):
        copy_x1(k).wait_send()

        @pl.when(jnp.logical_not(is_root))
        def _():
            copy_down(k).wait_send()

        for y0 in range(2):
            t = y0 * half + k

            @pl.when(same_core & same_x & (y == y0))
            def _():
                copy_x3(t, 2).wait_send()

            @pl.when(same_core & (y == y0))
            def _():
                copy_x3(t, 1).wait_send()

            @pl.when(same_core)
            def _():
                copy_x3(t, 0).wait_send()

            @pl.when(z != (0 if t < half else planes - 1))
            def _():
                copy_p(t).wait_send()

    @pl.when(is_end)
    def _():
        for d in range(1, n_dev):
            copy_f(d).wait_send()


def fused(n_seq, n_head, hidden_states, boundary, valid, pairs, w_first, b_first, w_second):
    traces, toks, feats = hidden_states.shape
    steps = boundary.shape[1]
    depth, width = w_first.shape
    half, cols = traces // 2, width // 2
    bf16, f32 = jnp.bfloat16, jnp.float32
    dma = pltpu.SemaphoreType.DMA
    vmem = pl.BlockSpec(memory_space=pltpu.VMEM)
    reward, score, margin = pl.pallas_call(
        functools.partial(kernel, n_seq, n_head),
        out_shape=(
            jax.ShapeDtypeStruct((traces, steps), f32),
            jax.ShapeDtypeStruct((traces, 1), f32),
            jax.ShapeDtypeStruct((pairs.shape[0], 1), f32),
        ),
        in_specs=[vmem] * 7,
        out_specs=(vmem,) * 3,
        scratch_shapes=[
            pltpu.VMEM((half, steps, feats), bf16),
            pltpu.VMEM((half, steps, feats), bf16),
            pltpu.VMEM((half, steps, feats), bf16),
            pltpu.VMEM((half, steps, feats), bf16),
            pltpu.VMEM((half, steps, feats), bf16),
            pltpu.VMEM((traces, steps, feats), bf16),
            pltpu.VMEM((depth, cols), bf16),
            pltpu.VMEM((2 * depth, cols), bf16),
            pltpu.VMEM((traces, steps, cols), f32),
            pltpu.VMEM((traces, steps, cols), f32),
            pltpu.VMEM((steps, 128), f32),
            pltpu.VMEM((4 * n_head, traces, steps), f32),
            dma((half,)), dma((half,)),
            dma, dma,
            dma((half,)), dma((half,)), dma((half,)),
            dma((traces, 3)), dma((traces,)),
            dma((traces,)), dma((traces,)),
            dma((n_seq * n_head,)), dma((4 * n_head,)),
        ],
        compiler_params=pltpu.CompilerParams(has_side_effects=True),
    )(
        hidden_states, boundary, valid, pairs, w_first,
        b_first.reshape(1, width), w_second.reshape(1, width),
    )
    return reward, score.reshape(traces), margin.reshape(pairs.shape[0])


def solution(mesh):
    n_seq, n_head = mesh.shape["seq"], mesh.shape["head"]
    paired = n_seq == 2 * n_head and n_head % 4 == 0
    body = functools.partial(fused, n_seq, n_head) if paired else per_device
    placed = (P(None, "seq", "head"), P(), P(), P(), P("seq", "head"), P("head"), P("head"))
    return jax.shard_map(
        body, mesh=mesh, in_specs=placed, out_specs=(P(), P(), P()), check_vma=False
    )
```

```python
import functools

import jax
import jax.numpy as jnp
from jax import lax
from jax.experimental import pallas as pl
from jax.experimental.pallas import tpu as pltpu
from jax.sharding import PartitionSpec as P

MESH = pl.DeviceIdType.MESH


def score_rows(rows, w_first, b_first, w_second):
    pre = jnp.dot(
        rows, lax.all_gather(w_first, "seq", axis=0, tiled=True), preferred_element_type=jnp.float32
    )
    return jnp.sum(jnp.maximum(pre + b_first, 0.0) * w_second, axis=-1)


def per_device(hidden_states, boundary, valid, pairs, w_first, b_first, w_second):
    traces, tok_dev, quarter = hidden_states.shape
    offset = lax.axis_index("seq") * tok_dev
    positions = offset + jnp.arange(tok_dev, dtype=jnp.int32)
    hits = boundary[:, :, None] == positions[None, None, :]
    whole = lax.all_gather(hidden_states, "head", axis=2, tiled=True)
    token_logit = score_rows(
        whole.reshape(traces * tok_dev, whole.shape[2]), w_first, b_first, w_second
    )
    token_logit = token_logit.reshape(traces, tok_dev)
    partial_logit = jnp.sum(jnp.where(hits, token_logit[:, None, :], 0.0), axis=2)
    logit = lax.psum(partial_logit, ("seq", "head"))
    live = valid == 1
    step_reward = jnp.where(live, logit, jnp.float32(0.0))
    trace_score = jnp.min(jnp.where(live, logit, jnp.float32(1e30)), axis=1)
    trace_ids = jnp.arange(traces, dtype=jnp.int32)[None, :]
    winner = jnp.sum(jnp.where(pairs[:, 0:1] == trace_ids, trace_score[None, :], 0.0), axis=1)
    loser = jnp.sum(jnp.where(pairs[:, 1:2] == trace_ids, trace_score[None, :], 0.0), axis=1)
    return (step_reward, trace_score, winner - loser)


def kernel(
    n_seq, n_head, hid, bnd, valid, pairs, w, b, w2, reward, score, margin,
    xout, xin, xacc, xup, xdn, xall, wown, wall, psend, precv, fsend, frecv,
    s_x1, r_x1, s_w, r_w, s_x2, r_up, r_dn, s_x3, r_x3, s_p, r_p, s_f, r_f,
):
    traces, toks, _ = hid.shape
    half = traces // 2
    planes = n_seq // 2
    depth = w.shape[0]
    cols = w.shape[1] // 2
    s = lax.axis_index("seq")
    h = lax.axis_index("head")
    z = s // 2
    y = s % 2
    other = 1 - y

    def remote(src, dst, send, recv, to_s, to_h):
        return pltpu.make_async_remote_copy(
            src_ref=src, dst_ref=dst, send_sem=send, recv_sem=recv,
            device_id=(to_s, to_h), device_id_type=MESH,
        )

    across = s + 1 - 2 * y
    h_core = h + 1 - 2 * (h % 2)
    h_x = lax.rem(h + 2, n_head)

    def pick(t):
        pos = lax.broadcasted_iota(jnp.int32, (toks, bnd.shape[1]), 0) + s * toks
        hot = jnp.where(bnd[pl.ds(t, 1), :] == pos, 1.0, 0.0).astype(jnp.bfloat16)
        got = lax.dot_general(
            hot, hid[t], (((0,), (0,)), ((), ())), preferred_element_type=jnp.float32
        )
        return got.astype(jnp.bfloat16)

    def copy_x1(k):
        return remote(xout.at[k], xin.at[k], s_x1.at[k], r_x1.at[k], across, h)

    def my_cols(which):
        return pl.ds(pl.multiple_of(which * cols, cols), cols)

    part = depth // 2

    def copy_w(i):
        rows = pl.ds(pl.multiple_of(y * depth + i * part, part), part)
        return remote(wown.at[pl.ds(i * part, part)], wall.at[rows], s_w.at[i], r_w.at[i], across, h)

    wown[...] = w[:, my_cols(other)]
    copy_w(0).start()
    for k in range(half):
        xout[k] = pick(other * half + k)
        copy_x1(k).start()
    copy_w(1).start()
    wall[pl.ds(pl.multiple_of(y * depth, depth), depth), :] = w[:, my_cols(y)]

    for k in range(half):
        xacc[k] = pick(y * half + k)

    same_core = (h % 2) == (z % 2)

    def copy_x3(t, way):
        to_s, to_h = ((s, h_core), (across, h), (s, h_x))[way]
        return remote(xall.at[t], xall.at[t], s_x3.at[t, way], r_x3.at[t], to_s, to_h)

    is_root = z == h
    from_up = (z >= h) & (z < planes - 1)
    from_dn = (z <= h) & (z > 0)

    def copy_down(k):
        return remote(xacc.at[k], xup.at[k], s_x2.at[k], r_up.at[k], lax.rem(s + n_seq - 2, n_seq), h)

    def copy_up(k):
        return remote(xacc.at[k], xdn.at[k], s_x2.at[k], r_dn.at[k], lax.rem(s + 2, n_seq), h)

    def chain(k):
        copy_x1(k).wait_recv()
        xacc[k] = xacc[k] + xin[k]

        @pl.when(from_up)
        def _():
            copy_down(k).wait_recv()
            xacc[k] = xacc[k] + xup[k]

        @pl.when(from_dn)
        def _():
            copy_up(k).wait_recv()
            xacc[k] = xacc[k] + xdn[k]

        @pl.when(z > h)
        def _():
            copy_down(k).start()

        @pl.when(z < h)
        def _():
            copy_up(k).start()

        @pl.when(is_root)
        def _():
            t = y * half + k
            xall[t] = xacc[k]
            copy_x3(t, 1).start()
            copy_x3(t, 2).start()
            copy_x3(t, 0).start()

    def spread(k):
        t = y * half + k

        @pl.when(jnp.logical_not(is_root))
        def _():
            copy_x3(t, 0).wait_recv()

            @pl.when(same_core)
            def _():
                copy_x3(t, 1).start()
                copy_x3(t, 0).start()

    def spread_far(k):
        t = other * half + k
        copy_x3(t, 0).wait_recv()

        @pl.when(same_core)
        def _():
            copy_x3(t, 0).start()

    for k in range(half):
        chain(k)
    for k in range(half):
        spread(k)
    for k in range(half):
        spread_far(k)
    for i in range(2):
        copy_w(i).wait_recv()

    def copy_p(t, down):
        to_s = lax.rem(s + n_seq - 2, n_seq) if down else lax.rem(s + 2, n_seq)
        return remote(psend.at[t], precv.at[t], s_p.at[t], r_p.at[t], to_s, h)

    bias = b[:, my_cols(y)]
    out_row = w2[:, my_cols(y)]
    lanes = lax.broadcasted_iota(jnp.int32, (xall.shape[1], 128), 1)
    fsend[...] = jnp.zeros_like(fsend)

    def reduce_step(tick, _):
        for down in (True, False):
            first = planes - 1 if down else 0
            last = planes - 1 - first
            k = tick - (planes - 1 - z if down else z)
            t = k if down else half + k

            @pl.when((k >= 0) & (k < half))
            def _():
                psend[t] = jnp.dot(xall[t], wall[...], preferred_element_type=jnp.float32)

                @pl.when(z != first)
                def _():
                    copy_p(t, down).wait_recv()
                    psend[t] = psend[t] + precv[t]

                @pl.when(z != last)
                def _():
                    copy_p(t, down).start()

                @pl.when(z == last)
                def _():
                    act = jnp.maximum(psend[t] + bias, 0.0) * out_row
                    total = jnp.sum(act, axis=1, keepdims=True)
                    fsend[...] = fsend[...] + jnp.where(lanes == t, total, 0.0)

        return 0

    lax.fori_loop(0, half + planes - 1, reduce_step, 0)

    is_end = (z == 0) | (z == planes - 1)
    slots = 4 * n_head
    me = s * n_head + h
    n_dev = n_seq * n_head
    slot = jnp.where(z == 0, 0, 1) * (2 * n_head) + y * n_head + h

    def copy_f(d):
        to = lax.rem(me + d, n_dev)
        return remote(
            frecv.at[slot], frecv.at[slot], s_f.at[d], r_f.at[slot], to // n_head, lax.rem(to, n_head)
        )

    @pl.when(is_end)
    def _():
        frecv[slot] = jnp.transpose(fsend[...])[: frecv.shape[1], :]
        for d in range(1, n_dev):
            copy_f(d).start()

    logit = jnp.zeros(frecv.shape[1:], jnp.float32)
    for i in range(slots):

        @pl.when(jnp.logical_not(is_end & (slot == i)))
        def _():
            remote(frecv.at[i], frecv.at[i], s_f.at[0], r_f.at[i], across, h).wait_recv()

        logit = logit + frecv[i]

    live = valid[...] == 1
    reward[...] = jnp.where(live, logit, 0.0)
    low = jnp.min(jnp.where(live, logit, 1e30), axis=1, keepdims=True)
    score[...] = low
    eye = lax.broadcasted_iota(jnp.int32, (traces, traces), 0) == lax.broadcasted_iota(
        jnp.int32, (traces, traces), 1
    )
    row = jnp.sum(jnp.where(eye, low, 0.0), axis=0, keepdims=True)
    ids = lax.broadcasted_iota(jnp.int32, (pairs.shape[0], traces), 1)
    winner = jnp.sum(jnp.where(pairs[:, 0:1] == ids, row, 0.0), axis=1, keepdims=True)
    loser = jnp.sum(jnp.where(pairs[:, 1:2] == ids, row, 0.0), axis=1, keepdims=True)
    margin[...] = winner - loser

    for i in range(2):
        copy_w(i).wait_send()
    for k in range(half):
        copy_x1(k).wait_send()

        @pl.when(jnp.logical_not(is_root))
        def _():
            copy_down(k).wait_send()

        for t, near in ((y * half + k, True), (other * half + k, False)):

            @pl.when(same_core)
            def _():
                copy_x3(t, 0).wait_send()
                if near:
                    copy_x3(t, 1).wait_send()

        @pl.when(is_root)
        def _():
            copy_x3(y * half + k, 2).wait_send()

        @pl.when(z != 0)
        def _():
            copy_p(k, True).wait_send()

        @pl.when(z != planes - 1)
        def _():
            copy_p(half + k, False).wait_send()

    @pl.when(is_end)
    def _():
        for d in range(1, n_dev):
            copy_f(d).wait_send()


def fused(n_seq, n_head, hidden_states, boundary, valid, pairs, w_first, b_first, w_second):
    traces, toks, feats = hidden_states.shape
    steps = boundary.shape[1]
    depth, width = w_first.shape
    half, cols = traces // 2, width // 2
    bf16, f32 = jnp.bfloat16, jnp.float32
    dma = pltpu.SemaphoreType.DMA
    vmem = pl.BlockSpec(memory_space=pltpu.VMEM)
    reward, score, margin = pl.pallas_call(
        functools.partial(kernel, n_seq, n_head),
        out_shape=(
            jax.ShapeDtypeStruct((traces, steps), f32),
            jax.ShapeDtypeStruct((traces, 1), f32),
            jax.ShapeDtypeStruct((pairs.shape[0], 1), f32),
        ),
        in_specs=[vmem] * 7,
        out_specs=(vmem,) * 3,
        scratch_shapes=[
            pltpu.VMEM((half, steps, feats), bf16),
            pltpu.VMEM((half, steps, feats), bf16),
            pltpu.VMEM((half, steps, feats), bf16),
            pltpu.VMEM((half, steps, feats), bf16),
            pltpu.VMEM((half, steps, feats), bf16),
            pltpu.VMEM((traces, steps, feats), bf16),
            pltpu.VMEM((depth, cols), bf16),
            pltpu.VMEM((2 * depth, cols), bf16),
            pltpu.VMEM((traces, steps, cols), f32),
            pltpu.VMEM((traces, steps, cols), f32),
            pltpu.VMEM((steps, 128), f32),
            pltpu.VMEM((4 * n_head, traces, steps), f32),
            dma((half,)), dma((half,)),
            dma((2,)), dma((2,)),
            dma((half,)), dma((half,)), dma((half,)),
            dma((traces, 3)), dma((traces,)),
            dma((traces,)), dma((traces,)),
            dma((n_seq * n_head,)), dma((4 * n_head,)),
        ],
        compiler_params=pltpu.CompilerParams(has_side_effects=True),
    )(
        hidden_states, boundary, valid, pairs, w_first,
        b_first.reshape(1, width), w_second.reshape(1, width),
    )
    return reward, score.reshape(traces), margin.reshape(pairs.shape[0])


def solution(mesh):
    n_seq, n_head = mesh.shape["seq"], mesh.shape["head"]
    paired = n_seq == 2 * n_head and n_head % 4 == 0
    body = functools.partial(fused, n_seq, n_head) if paired else per_device
    placed = (P(None, "seq", "head"), P(), P(), P(), P("seq", "head"), P("head"), P("head"))
    return jax.shard_map(
        body, mesh=mesh, in_specs=placed, out_specs=(P(), P(), P()), check_vma=False
    )
```

```python
import functools

import jax
import jax.numpy as jnp
from jax import lax
from jax.experimental import pallas as pl
from jax.experimental.pallas import tpu as pltpu
from jax.sharding import PartitionSpec as P

MESH = pl.DeviceIdType.MESH


def score_rows(rows, w_first, b_first, w_second):
    pre = jnp.dot(
        rows, lax.all_gather(w_first, "seq", axis=0, tiled=True), preferred_element_type=jnp.float32
    )
    return jnp.sum(jnp.maximum(pre + b_first, 0.0) * w_second, axis=-1)


def per_device(hidden_states, boundary, valid, pairs, w_first, b_first, w_second):
    traces, tok_dev, quarter = hidden_states.shape
    offset = lax.axis_index("seq") * tok_dev
    positions = offset + jnp.arange(tok_dev, dtype=jnp.int32)
    hits = boundary[:, :, None] == positions[None, None, :]
    whole = lax.all_gather(hidden_states, "head", axis=2, tiled=True)
    token_logit = score_rows(
        whole.reshape(traces * tok_dev, whole.shape[2]), w_first, b_first, w_second
    )
    token_logit = token_logit.reshape(traces, tok_dev)
    partial_logit = jnp.sum(jnp.where(hits, token_logit[:, None, :], 0.0), axis=2)
    logit = lax.psum(partial_logit, ("seq", "head"))
    live = valid == 1
    step_reward = jnp.where(live, logit, jnp.float32(0.0))
    trace_score = jnp.min(jnp.where(live, logit, jnp.float32(1e30)), axis=1)
    trace_ids = jnp.arange(traces, dtype=jnp.int32)[None, :]
    winner = jnp.sum(jnp.where(pairs[:, 0:1] == trace_ids, trace_score[None, :], 0.0), axis=1)
    loser = jnp.sum(jnp.where(pairs[:, 1:2] == trace_ids, trace_score[None, :], 0.0), axis=1)
    return (step_reward, trace_score, winner - loser)


def kernel(
    n_seq, n_head, hid, bnd, valid, pairs, w, b, w2, reward, score, margin,
    xout, xin, xacc, xup, xdn, xall, wown, wall, psend, precv, fsend, frecv,
    s_x1, r_x1, s_w, r_w, s_x2, r_up, r_dn, s_x3, r_x3, s_p, r_p, s_f, r_f,
):
    traces, toks, _ = hid.shape
    half = traces
    block = bnd.shape[1] // 2
    planes = n_seq // 2
    depth = w.shape[0]
    cols = w.shape[1] // 2
    s = lax.axis_index("seq")
    h = lax.axis_index("head")
    z = s // 2
    y = s % 2
    other = 1 - y

    def remote(src, dst, send, recv, to_s, to_h):
        return pltpu.make_async_remote_copy(
            src_ref=src, dst_ref=dst, send_sem=send, recv_sem=recv,
            device_id=(to_s, to_h), device_id_type=MESH,
        )

    across = s + 1 - 2 * y
    h_core = h + 1 - 2 * (h % 2)
    h_x = lax.rem(h + 2, n_head)

    barrier = pltpu.get_barrier_semaphore()

    def greet(to_s, to_h):
        pl.semaphore_signal(barrier, inc=1, device_id=(to_s, to_h), device_id_type=MESH)

    greet(across, h)
    greet(s, h_core)
    greet(s, h_x)

    @pl.when(z > 0)
    def _():
        greet(s - 2, h)

    @pl.when(z < planes - 1)
    def _():
        greet(s + 2, h)

    def pick(t):
        pos = lax.broadcasted_iota(jnp.int32, (toks, bnd.shape[1]), 0) + s * toks
        hot = jnp.where(bnd[pl.ds(t, 1), :] == pos, 1.0, 0.0).astype(jnp.bfloat16)
        got = lax.dot_general(
            hot, hid[t], (((0,), (0,)), ((), ())), preferred_element_type=jnp.float32
        )
        return got.astype(jnp.bfloat16)

    def copy_x1(k):
        return remote(xout.at[k], xin.at[k], s_x1.at[k], r_x1.at[k], across, h)

    def my_cols(which):
        return pl.ds(pl.multiple_of(which * cols, cols), cols)

    part = depth // 2

    def copy_w(i):
        rows = pl.ds(pl.multiple_of(y * depth + i * part, part), part)
        return remote(wown.at[pl.ds(i * part, part)], wall.at[rows], s_w.at[i], r_w.at[i], across, h)

    def pick_half(which, dst):
        for i in range(traces // 2):
            got = pick(which * (traces // 2) + i)
            dst[2 * i] = got[:block]
            dst[2 * i + 1] = got[block:]

    pick_half(other, xout)
    wown[...] = w[:, my_cols(other)]
    pl.semaphore_wait(
        barrier, 3 + jnp.where(z > 0, 1, 0) + jnp.where(z < planes - 1, 1, 0)
    )
    for k in range(half):
        copy_x1(k).start()
    for i in range(2):
        copy_w(i).start()
    wall[pl.ds(pl.multiple_of(y * depth, depth), depth), :] = w[:, my_cols(y)]

    pick_half(y, xacc)

    same_core = (h % 2) == (z % 2)

    def copy_x3(t, way):
        to_s, to_h = ((s, h_core), (across, h), (s, h_x))[way]
        return remote(xall.at[t], xall.at[t], s_x3.at[t, way], r_x3.at[t], to_s, to_h)

    is_root = z == h
    from_up = (z >= h) & (z < planes - 1)
    from_dn = (z <= h) & (z > 0)

    def copy_down(k):
        return remote(xacc.at[k], xup.at[k], s_x2.at[k], r_up.at[k], lax.rem(s + n_seq - 2, n_seq), h)

    def copy_up(k):
        return remote(xacc.at[k], xdn.at[k], s_x2.at[k], r_dn.at[k], lax.rem(s + 2, n_seq), h)

    def chain(k):
        copy_x1(k).wait_recv()
        xacc[k] = xacc[k] + xin[k]

        @pl.when(from_up)
        def _():
            copy_down(k).wait_recv()
            xacc[k] = xacc[k] + xup[k]

        @pl.when(from_dn)
        def _():
            copy_up(k).wait_recv()
            xacc[k] = xacc[k] + xdn[k]

        @pl.when(z > h)
        def _():
            copy_down(k).start()

        @pl.when(z < h)
        def _():
            copy_up(k).start()

        @pl.when(is_root)
        def _():
            t = y * half + k
            xall[t] = xacc[k]
            copy_x3(t, 1).start()
            copy_x3(t, 2).start()
            copy_x3(t, 0).start()

    def spread(k):
        t = y * half + k

        @pl.when(jnp.logical_not(is_root))
        def _():
            copy_x3(t, 0).wait_recv()

            @pl.when(same_core)
            def _():
                copy_x3(t, 1).start()
                copy_x3(t, 0).start()

    def spread_far(k):
        t = other * half + k
        copy_x3(t, 0).wait_recv()

        @pl.when(same_core)
        def _():
            copy_x3(t, 0).start()

    for k in range(half):
        chain(k)
    def copy_p(t, down):
        to_s = lax.rem(s + n_seq - 2, n_seq) if down else lax.rem(s + 2, n_seq)
        return remote(psend.at[t], precv.at[t], s_p.at[t], r_p.at[t], to_s, h)

    bias = b[:, my_cols(y)]
    out_row = w2[:, my_cols(y)]
    lanes = lax.broadcasted_iota(jnp.int32, (block, 128), 1)
    fsend[...] = jnp.zeros_like(fsend)

    def reduce_step(tick):
        for down in (True, False):
            first = planes - 1 if down else 0
            last = planes - 1 - first
            k = tick - (planes - 1 - z if down else z)
            t = k if down else half + k

            @pl.when((k >= 0) & (k < half))
            def _():
                psend[t] = jnp.dot(xall[t], wall[...], preferred_element_type=jnp.float32)

                @pl.when(z != first)
                def _():
                    copy_p(t, down).wait_recv()
                    psend[t] = psend[t] + precv[t]

                @pl.when(z != last)
                def _():
                    copy_p(t, down).start()

                @pl.when(z == last)
                def _():
                    act = jnp.maximum(psend[t] + bias, 0.0) * out_row
                    total = jnp.sum(act, axis=1, keepdims=True)
                    here = pl.ds(pl.multiple_of((k % 2) * block, block), block)
                    fsend[here, :] = fsend[here, :] + jnp.where(lanes == t // 2, total, 0.0)

    for k in range(half):
        spread(k)
        spread_far(k)
        if k == 0:
            for i in range(2):
                copy_w(i).wait_recv()
        reduce_step(k)
    for k in range(half, half + planes - 1):
        reduce_step(k)

    is_end = (z == 0) | (z == planes - 1)
    slots = 4 * n_head
    me = s * n_head + h
    n_dev = n_seq * n_head
    slot = jnp.where(z == 0, 0, 1) * (2 * n_head) + y * n_head + h

    def copy_f(d):
        to = lax.rem(me + d, n_dev)
        return remote(
            frecv.at[slot], frecv.at[slot], s_f.at[d], r_f.at[slot], to // n_head, lax.rem(to, n_head)
        )

    @pl.when(is_end)
    def _():
        frecv[slot] = jnp.transpose(fsend[...])[: frecv.shape[1], :]
        for d in range(1, n_dev):
            copy_f(d).start()

    logit = jnp.zeros(frecv.shape[1:], jnp.float32)
    for i in range(slots):

        @pl.when(jnp.logical_not(is_end & (slot == i)))
        def _():
            remote(frecv.at[i], frecv.at[i], s_f.at[0], r_f.at[i], across, h).wait_recv()

        logit = logit + frecv[i]

    live = valid[...] == 1
    reward[...] = jnp.where(live, logit, 0.0)
    low = jnp.min(jnp.where(live, logit, 1e30), axis=1, keepdims=True)
    score[...] = low
    eye = lax.broadcasted_iota(jnp.int32, (traces, traces), 0) == lax.broadcasted_iota(
        jnp.int32, (traces, traces), 1
    )
    row = jnp.sum(jnp.where(eye, low, 0.0), axis=0, keepdims=True)
    ids = lax.broadcasted_iota(jnp.int32, (pairs.shape[0], traces), 1)
    winner = jnp.sum(jnp.where(pairs[:, 0:1] == ids, row, 0.0), axis=1, keepdims=True)
    loser = jnp.sum(jnp.where(pairs[:, 1:2] == ids, row, 0.0), axis=1, keepdims=True)
    margin[...] = winner - loser

    for i in range(2):
        copy_w(i).wait_send()
    for k in range(half):
        copy_x1(k).wait_send()

        @pl.when(jnp.logical_not(is_root))
        def _():
            copy_down(k).wait_send()

        for t, near in ((y * half + k, True), (other * half + k, False)):

            @pl.when(same_core)
            def _():
                copy_x3(t, 0).wait_send()
                if near:
                    copy_x3(t, 1).wait_send()

        @pl.when(is_root)
        def _():
            copy_x3(y * half + k, 2).wait_send()

        @pl.when(z != 0)
        def _():
            copy_p(k, True).wait_send()

        @pl.when(z != planes - 1)
        def _():
            copy_p(half + k, False).wait_send()

    @pl.when(is_end)
    def _():
        for d in range(1, n_dev):
            copy_f(d).wait_send()


def fused(n_seq, n_head, hidden_states, boundary, valid, pairs, w_first, b_first, w_second):
    traces, toks, feats = hidden_states.shape
    steps = boundary.shape[1]
    depth, width = w_first.shape
    half, block, cols = traces, steps // 2, width // 2
    bf16, f32 = jnp.bfloat16, jnp.float32
    dma = pltpu.SemaphoreType.DMA
    vmem = pl.BlockSpec(memory_space=pltpu.VMEM)
    reward, score, margin = pl.pallas_call(
        functools.partial(kernel, n_seq, n_head),
        out_shape=(
            jax.ShapeDtypeStruct((traces, steps), f32),
            jax.ShapeDtypeStruct((traces, 1), f32),
            jax.ShapeDtypeStruct((pairs.shape[0], 1), f32),
        ),
        in_specs=[vmem] * 7,
        out_specs=(vmem,) * 3,
        scratch_shapes=[
            pltpu.VMEM((half, block, feats), bf16),
            pltpu.VMEM((half, block, feats), bf16),
            pltpu.VMEM((half, block, feats), bf16),
            pltpu.VMEM((half, block, feats), bf16),
            pltpu.VMEM((half, block, feats), bf16),
            pltpu.VMEM((2 * half, block, feats), bf16),
            pltpu.VMEM((depth, cols), bf16),
            pltpu.VMEM((2 * depth, cols), bf16),
            pltpu.VMEM((2 * half, block, cols), f32),
            pltpu.VMEM((2 * half, block, cols), f32),
            pltpu.VMEM((steps, 128), f32),
            pltpu.VMEM((4 * n_head, traces, steps), f32),
            dma((half,)), dma((half,)),
            dma((2,)), dma((2,)),
            dma((half,)), dma((half,)), dma((half,)),
            dma((2 * half, 3)), dma((2 * half,)),
            dma((2 * half,)), dma((2 * half,)),
            dma((n_seq * n_head,)), dma((4 * n_head,)),
        ],
        compiler_params=pltpu.CompilerParams(collective_id=0, has_side_effects=True),
    )(
        hidden_states, boundary, valid, pairs, w_first,
        b_first.reshape(1, width), w_second.reshape(1, width),
    )
    return reward, score.reshape(traces), margin.reshape(pairs.shape[0])


def solution(mesh):
    n_seq, n_head = mesh.shape["seq"], mesh.shape["head"]
    paired = n_seq == 2 * n_head and n_head % 4 == 0
    body = functools.partial(fused, n_seq, n_head) if paired else per_device
    placed = (P(None, "seq", "head"), P(), P(), P(), P("seq", "head"), P("head"), P("head"))
    return jax.shard_map(
        body, mesh=mesh, in_specs=placed, out_specs=(P(), P(), P()), check_vma=False
    )
```

```python
import functools

import jax
import jax.numpy as jnp
from jax import lax
from jax.experimental import pallas as pl
from jax.experimental.pallas import tpu as pltpu
from jax.sharding import PartitionSpec as P

MESH = pl.DeviceIdType.MESH


def score_rows(rows, w_first, b_first, w_second):
    pre = jnp.dot(
        rows, lax.all_gather(w_first, "seq", axis=0, tiled=True), preferred_element_type=jnp.float32
    )
    return jnp.sum(jnp.maximum(pre + b_first, 0.0) * w_second, axis=-1)


def per_device(hidden_states, boundary, valid, pairs, w_first, b_first, w_second):
    traces, tok_dev, quarter = hidden_states.shape
    offset = lax.axis_index("seq") * tok_dev
    positions = offset + jnp.arange(tok_dev, dtype=jnp.int32)
    hits = boundary[:, :, None] == positions[None, None, :]
    whole = lax.all_gather(hidden_states, "head", axis=2, tiled=True)
    token_logit = score_rows(
        whole.reshape(traces * tok_dev, whole.shape[2]), w_first, b_first, w_second
    )
    token_logit = token_logit.reshape(traces, tok_dev)
    partial_logit = jnp.sum(jnp.where(hits, token_logit[:, None, :], 0.0), axis=2)
    logit = lax.psum(partial_logit, ("seq", "head"))
    live = valid == 1
    step_reward = jnp.where(live, logit, jnp.float32(0.0))
    trace_score = jnp.min(jnp.where(live, logit, jnp.float32(1e30)), axis=1)
    trace_ids = jnp.arange(traces, dtype=jnp.int32)[None, :]
    winner = jnp.sum(jnp.where(pairs[:, 0:1] == trace_ids, trace_score[None, :], 0.0), axis=1)
    loser = jnp.sum(jnp.where(pairs[:, 1:2] == trace_ids, trace_score[None, :], 0.0), axis=1)
    return (step_reward, trace_score, winner - loser)


def kernel(
    n_seq, n_head, hid_hbm, bnd, valid, pairs, w_hbm, b, w2, reward, score, margin,
    hid, w, s_hid, s_win,
    xout, xin, xacc, xup, xdn, xall, wown, wall, psend, precv, fsend, frecv,
    s_x1, r_x1, s_w, r_w, s_x2, r_up, r_dn, s_x3, r_x3, s_p, r_p, s_f, r_f,
):
    fetch_hid = pltpu.make_async_copy(hid_hbm, hid, s_hid)
    fetch_w = pltpu.make_async_copy(w_hbm, w, s_win)
    fetch_hid.start()
    fetch_w.start()
    traces, toks, _ = hid.shape
    half = traces
    block = bnd.shape[1] // 2
    planes = n_seq // 2
    depth = w.shape[0]
    cols = w.shape[1] // 2
    s = lax.axis_index("seq")
    h = lax.axis_index("head")
    z = s // 2
    y = s % 2
    other = 1 - y

    def remote(src, dst, send, recv, to_s, to_h):
        return pltpu.make_async_remote_copy(
            src_ref=src, dst_ref=dst, send_sem=send, recv_sem=recv,
            device_id=(to_s, to_h), device_id_type=MESH,
        )

    across = s + 1 - 2 * y
    h_core = h + 1 - 2 * (h % 2)
    h_x = lax.rem(h + 2, n_head)

    barrier = pltpu.get_barrier_semaphore()

    def greet(to_s, to_h):
        pl.semaphore_signal(barrier, inc=1, device_id=(to_s, to_h), device_id_type=MESH)

    greet(across, h)
    greet(s, h_core)
    greet(s, h_x)

    @pl.when(z > 0)
    def _():
        greet(s - 2, h)

    @pl.when(z < planes - 1)
    def _():
        greet(s + 2, h)

    def pick(t):
        pos = lax.broadcasted_iota(jnp.int32, (toks, bnd.shape[1]), 0) + s * toks
        hot = jnp.where(bnd[pl.ds(t, 1), :] == pos, 1.0, 0.0).astype(jnp.bfloat16)
        got = lax.dot_general(
            hot, hid[t], (((0,), (0,)), ((), ())), preferred_element_type=jnp.float32
        )
        return got.astype(jnp.bfloat16)

    def copy_x1(k):
        return remote(xout.at[k], xin.at[k], s_x1.at[k], r_x1.at[k], across, h)

    def my_cols(which):
        return pl.ds(pl.multiple_of(which * cols, cols), cols)

    part = depth // 2

    def copy_w(i):
        rows = pl.ds(pl.multiple_of(y * depth + i * part, part), part)
        return remote(wown.at[pl.ds(i * part, part)], wall.at[rows], s_w.at[i], r_w.at[i], across, h)

    def pick_half(which, dst):
        for i in range(traces // 2):
            got = pick(which * (traces // 2) + i)
            dst[2 * i] = got[:block]
            dst[2 * i + 1] = got[block:]

    fetch_hid.wait()
    pick_half(other, xout)
    pl.semaphore_wait(
        barrier, 3 + jnp.where(z > 0, 1, 0) + jnp.where(z < planes - 1, 1, 0)
    )
    for k in range(half):
        copy_x1(k).start()
    fetch_w.wait()
    wown[...] = w[:, my_cols(other)]
    for i in range(2):
        copy_w(i).start()
    wall[pl.ds(pl.multiple_of(y * depth, depth), depth), :] = w[:, my_cols(y)]

    pick_half(y, xacc)

    same_core = (h % 2) == (z % 2)

    def copy_x3(t, way):
        to_s, to_h = ((s, h_core), (across, h), (s, h_x))[way]
        return remote(xall.at[t], xall.at[t], s_x3.at[t, way], r_x3.at[t], to_s, to_h)

    is_root = z == h
    from_up = (z >= h) & (z < planes - 1)
    from_dn = (z <= h) & (z > 0)

    def copy_down(k):
        return remote(xacc.at[k], xup.at[k], s_x2.at[k], r_up.at[k], lax.rem(s + n_seq - 2, n_seq), h)

    def copy_up(k):
        return remote(xacc.at[k], xdn.at[k], s_x2.at[k], r_dn.at[k], lax.rem(s + 2, n_seq), h)

    def chain(k):
        copy_x1(k).wait_recv()
        xacc[k] = xacc[k] + xin[k]

        @pl.when(from_up)
        def _():
            copy_down(k).wait_recv()
            xacc[k] = xacc[k] + xup[k]

        @pl.when(from_dn)
        def _():
            copy_up(k).wait_recv()
            xacc[k] = xacc[k] + xdn[k]

        @pl.when(z > h)
        def _():
            copy_down(k).start()

        @pl.when(z < h)
        def _():
            copy_up(k).start()

        @pl.when(is_root)
        def _():
            t = y * half + k
            xall[t] = xacc[k]
            copy_x3(t, 1).start()
            copy_x3(t, 2).start()
            copy_x3(t, 0).start()

    def spread(k):
        t = y * half + k

        @pl.when(jnp.logical_not(is_root))
        def _():
            copy_x3(t, 0).wait_recv()

            @pl.when(same_core)
            def _():
                copy_x3(t, 1).start()
                copy_x3(t, 0).start()

    def spread_far(k):
        t = other * half + k
        copy_x3(t, 0).wait_recv()

        @pl.when(same_core)
        def _():
            copy_x3(t, 0).start()

    for k in range(half):
        chain(k)
    def copy_p(t, down):
        to_s = lax.rem(s + n_seq - 2, n_seq) if down else lax.rem(s + 2, n_seq)
        return remote(psend.at[t], precv.at[t], s_p.at[t], r_p.at[t], to_s, h)

    bias = b[:, my_cols(y)]
    out_row = w2[:, my_cols(y)]
    lanes = lax.broadcasted_iota(jnp.int32, (block, 128), 1)
    fsend[...] = jnp.zeros_like(fsend)

    def reduce_step(tick):
        for down in (True, False):
            first = planes - 1 if down else 0
            last = planes - 1 - first
            k = tick - (planes - 1 - z if down else z)
            t = k if down else half + k

            @pl.when((k >= 0) & (k < half))
            def _():
                psend[t] = jnp.dot(xall[t], wall[...], preferred_element_type=jnp.float32)

                @pl.when(z != first)
                def _():
                    copy_p(t, down).wait_recv()
                    psend[t] = psend[t] + precv[t]

                @pl.when(z != last)
                def _():
                    copy_p(t, down).start()

                @pl.when(z == last)
                def _():
                    act = jnp.maximum(psend[t] + bias, 0.0) * out_row
                    total = jnp.sum(act, axis=1, keepdims=True)
                    here = pl.ds(pl.multiple_of((k % 2) * block, block), block)
                    fsend[here, :] = fsend[here, :] + jnp.where(lanes == t // 2, total, 0.0)

    for k in range(half):
        spread(k)
    for k in range(half):
        spread_far(k)
        if k == 0:
            for i in range(2):
                copy_w(i).wait_recv()
        reduce_step(k)
    for k in range(half, half + planes - 1):
        reduce_step(k)

    is_end = (z == 0) | (z == planes - 1)
    slots = 4 * n_head
    me = s * n_head + h
    n_dev = n_seq * n_head
    slot = jnp.where(z == 0, 0, 1) * (2 * n_head) + y * n_head + h

    def copy_f(d):
        to = lax.rem(me + d, n_dev)
        return remote(
            frecv.at[slot], frecv.at[slot], s_f.at[d], r_f.at[slot], to // n_head, lax.rem(to, n_head)
        )

    @pl.when(is_end)
    def _():
        frecv[slot] = jnp.transpose(fsend[...])[: frecv.shape[1], :]
        for d in range(1, n_dev):
            copy_f(d).start()

    logit = jnp.zeros(frecv.shape[1:], jnp.float32)
    for i in range(slots):

        @pl.when(jnp.logical_not(is_end & (slot == i)))
        def _():
            remote(frecv.at[i], frecv.at[i], s_f.at[0], r_f.at[i], across, h).wait_recv()

        logit = logit + frecv[i]

    live = valid[...] == 1
    reward[...] = jnp.where(live, logit, 0.0)
    low = jnp.min(jnp.where(live, logit, 1e30), axis=1, keepdims=True)
    square = (traces, traces)
    eye = lax.broadcasted_iota(jnp.int32, square, 0) == lax.broadcasted_iota(jnp.int32, square, 1)
    score[...] = jnp.sum(jnp.where(eye, low, 0.0), axis=0)
    ids = lax.broadcasted_iota(jnp.int32, (traces, pairs.shape[1]), 0)
    winner = jnp.sum(jnp.where(pairs[0:1, :] == ids, low, 0.0), axis=0)
    loser = jnp.sum(jnp.where(pairs[1:2, :] == ids, low, 0.0), axis=0)
    margin[...] = winner - loser

    for i in range(2):
        copy_w(i).wait_send()
    for k in range(half):
        copy_x1(k).wait_send()

        @pl.when(jnp.logical_not(is_root))
        def _():
            copy_down(k).wait_send()

        for t, near in ((y * half + k, True), (other * half + k, False)):

            @pl.when(same_core)
            def _():
                copy_x3(t, 0).wait_send()
                if near:
                    copy_x3(t, 1).wait_send()

        @pl.when(is_root)
        def _():
            copy_x3(y * half + k, 2).wait_send()

        @pl.when(z != 0)
        def _():
            copy_p(k, True).wait_send()

        @pl.when(z != planes - 1)
        def _():
            copy_p(half + k, False).wait_send()

    @pl.when(is_end)
    def _():
        for d in range(1, n_dev):
            copy_f(d).wait_send()


def fused(n_seq, n_head, hidden_states, boundary, valid, pairs, w_first, b_first, w_second):
    traces, toks, feats = hidden_states.shape
    steps = boundary.shape[1]
    depth, width = w_first.shape
    half, block, cols = traces, steps // 2, width // 2
    bf16, f32 = jnp.bfloat16, jnp.float32
    dma = pltpu.SemaphoreType.DMA
    vmem = pl.BlockSpec(memory_space=pltpu.VMEM)
    hbm = pl.BlockSpec(memory_space=pl.ANY)
    return pl.pallas_call(
        functools.partial(kernel, n_seq, n_head),
        out_shape=(
            jax.ShapeDtypeStruct((traces, steps), f32),
            jax.ShapeDtypeStruct((traces,), f32),
            jax.ShapeDtypeStruct((pairs.shape[0],), f32),
        ),
        in_specs=[hbm] + [vmem] * 3 + [hbm] + [vmem] * 2,
        out_specs=(vmem,) * 3,
        scratch_shapes=[
            pltpu.VMEM((traces, toks, feats), bf16),
            pltpu.VMEM((depth, width), bf16),
            dma, dma,
            pltpu.VMEM((half, block, feats), bf16),
            pltpu.VMEM((half, block, feats), bf16),
            pltpu.VMEM((half, block, feats), bf16),
            pltpu.VMEM((half, block, feats), bf16),
            pltpu.VMEM((half, block, feats), bf16),
            pltpu.VMEM((2 * half, block, feats), bf16),
            pltpu.VMEM((depth, cols), bf16),
            pltpu.VMEM((2 * depth, cols), bf16),
            pltpu.VMEM((2 * half, block, cols), f32),
            pltpu.VMEM((2 * half, block, cols), f32),
            pltpu.VMEM((steps, 128), f32),
            pltpu.VMEM((4 * n_head, traces, steps), f32),
            dma((half,)), dma((half,)),
            dma((2,)), dma((2,)),
            dma((half,)), dma((half,)), dma((half,)),
            dma((2 * half, 3)), dma((2 * half,)),
            dma((2 * half,)), dma((2 * half,)),
            dma((n_seq * n_head,)), dma((4 * n_head,)),
        ],
        compiler_params=pltpu.CompilerParams(collective_id=0, has_side_effects=True),
    )(
        hidden_states, boundary, valid, pairs.T, w_first,
        b_first.reshape(1, width), w_second.reshape(1, width),
    )


def solution(mesh):
    n_seq, n_head = mesh.shape["seq"], mesh.shape["head"]
    paired = n_seq == 2 * n_head and n_head % 4 == 0
    body = functools.partial(fused, n_seq, n_head) if paired else per_device
    placed = (P(None, "seq", "head"), P(), P(), P(), P("seq", "head"), P("head"), P("head"))
    return jax.shard_map(
        body, mesh=mesh, in_specs=placed, out_specs=(P(), P(), P()), check_vma=False
    )
```

```python
import functools

import jax
import jax.numpy as jnp
from jax import lax
from jax.experimental import pallas as pl
from jax.experimental.pallas import tpu as pltpu
from jax.sharding import PartitionSpec as P

MESH = pl.DeviceIdType.MESH


def score_rows(rows, w_first, b_first, w_second):
    pre = jnp.dot(
        rows, lax.all_gather(w_first, "seq", axis=0, tiled=True), preferred_element_type=jnp.float32
    )
    return jnp.sum(jnp.maximum(pre + b_first, 0.0) * w_second, axis=-1)


def per_device(hidden_states, boundary, valid, pairs, w_first, b_first, w_second):
    traces, tok_dev, quarter = hidden_states.shape
    offset = lax.axis_index("seq") * tok_dev
    positions = offset + jnp.arange(tok_dev, dtype=jnp.int32)
    hits = boundary[:, :, None] == positions[None, None, :]
    whole = lax.all_gather(hidden_states, "head", axis=2, tiled=True)
    token_logit = score_rows(
        whole.reshape(traces * tok_dev, whole.shape[2]), w_first, b_first, w_second
    )
    token_logit = token_logit.reshape(traces, tok_dev)
    partial_logit = jnp.sum(jnp.where(hits, token_logit[:, None, :], 0.0), axis=2)
    logit = lax.psum(partial_logit, ("seq", "head"))
    live = valid == 1
    step_reward = jnp.where(live, logit, jnp.float32(0.0))
    trace_score = jnp.min(jnp.where(live, logit, jnp.float32(1e30)), axis=1)
    trace_ids = jnp.arange(traces, dtype=jnp.int32)[None, :]
    winner = jnp.sum(jnp.where(pairs[:, 0:1] == trace_ids, trace_score[None, :], 0.0), axis=1)
    loser = jnp.sum(jnp.where(pairs[:, 1:2] == trace_ids, trace_score[None, :], 0.0), axis=1)
    return (step_reward, trace_score, winner - loser)


def kernel(
    n_seq, n_head, hid_hbm, bnd, valid, pairs, w_hbm, b, w2, reward, score, margin,
    hid, w, s_hid, s_win,
    xout, xin, xacc, xup, xdn, xall, wown, wall, psend, precv, fsend, frecv,
    s_x1, r_x1, s_w, r_w, s_x2, r_up, r_dn, s_x3, r_x3, s_p, r_p, s_f, r_f,
):
    fetch_hid = pltpu.make_async_copy(hid_hbm, hid, s_hid)
    fetch_w = pltpu.make_async_copy(w_hbm, w, s_win)
    fetch_hid.start()
    fetch_w.start()
    traces, toks, _ = hid.shape
    half = traces
    block = bnd.shape[1] // 2
    planes = n_seq // 2
    depth = w.shape[0]
    cols = w.shape[1] // 2
    s = lax.axis_index("seq")
    h = lax.axis_index("head")
    z = s // 2
    y = s % 2
    other = 1 - y

    def remote(src, dst, send, recv, to_s, to_h):
        return pltpu.make_async_remote_copy(
            src_ref=src, dst_ref=dst, send_sem=send, recv_sem=recv,
            device_id=(to_s, to_h), device_id_type=MESH,
        )

    across = s + 1 - 2 * y
    h_core = h + 1 - 2 * (h % 2)
    h_x = lax.rem(h + 2, n_head)

    barrier = pltpu.get_barrier_semaphore()

    def greet(to_s, to_h):
        pl.semaphore_signal(barrier, inc=1, device_id=(to_s, to_h), device_id_type=MESH)

    greet(across, h)
    greet(s, h_core)
    greet(s, h_x)

    @pl.when(z > 0)
    def _():
        greet(s - 2, h)

    @pl.when(z < planes - 1)
    def _():
        greet(s + 2, h)

    def pick(t):
        pos = lax.broadcasted_iota(jnp.int32, (toks, bnd.shape[1]), 0) + s * toks
        hot = jnp.where(bnd[pl.ds(t, 1), :] == pos, 1.0, 0.0).astype(jnp.bfloat16)
        got = lax.dot_general(
            hot, hid[t], (((0,), (0,)), ((), ())), preferred_element_type=jnp.float32
        )
        return got.astype(jnp.bfloat16)

    def copy_x1(k):
        return remote(xout.at[k], xin.at[k], s_x1.at[k], r_x1.at[k], across, h)

    def my_cols(which):
        return pl.ds(pl.multiple_of(which * cols, cols), cols)

    part = depth // 2

    def copy_w(i):
        rows = pl.ds(pl.multiple_of(y * depth + i * part, part), part)
        return remote(wown.at[pl.ds(i * part, part)], wall.at[rows], s_w.at[i], r_w.at[i], across, h)

    def pick_half(which, dst):
        for i in range(traces // 2):
            got = pick(which * (traces // 2) + i)
            dst[2 * i] = got[:block]
            dst[2 * i + 1] = got[block:]

    fetch_hid.wait()
    pick_half(other, xout)
    pl.semaphore_wait(
        barrier, 3 + jnp.where(z > 0, 1, 0) + jnp.where(z < planes - 1, 1, 0)
    )
    for k in range(half):
        copy_x1(k).start()
    fetch_w.wait()
    wown[...] = w[:, my_cols(other)]
    for i in range(2):
        copy_w(i).start()
    wall[pl.ds(pl.multiple_of(y * depth, depth), depth), :] = w[:, my_cols(y)]

    pick_half(y, xacc)

    same_core = (h % 2) == (z % 2)

    def copy_x3(t, way):
        to_s, to_h = ((s, h_core), (across, h), (s, h_x))[way]
        return remote(xall.at[t], xall.at[t], s_x3.at[t, way], r_x3.at[t], to_s, to_h)

    is_root = z == h
    from_up = (z >= h) & (z < planes - 1)
    from_dn = (z <= h) & (z > 0)

    def copy_down(k):
        return remote(xacc.at[k], xup.at[k], s_x2.at[k], r_up.at[k], lax.rem(s + n_seq - 2, n_seq), h)

    def copy_up(k):
        return remote(xacc.at[k], xdn.at[k], s_x2.at[k], r_dn.at[k], lax.rem(s + 2, n_seq), h)

    def chain(k):
        copy_x1(k).wait_recv()
        xacc[k] = xacc[k] + xin[k]

        @pl.when(from_up)
        def _():
            copy_down(k).wait_recv()
            xacc[k] = xacc[k] + xup[k]

        @pl.when(from_dn)
        def _():
            copy_up(k).wait_recv()
            xacc[k] = xacc[k] + xdn[k]

        @pl.when(z > h)
        def _():
            copy_down(k).start()

        @pl.when(z < h)
        def _():
            copy_up(k).start()

        @pl.when(is_root)
        def _():
            t = y * half + k
            xall[t] = xacc[k]
            copy_x3(t, 1).start()
            copy_x3(t, 2).start()
            copy_x3(t, 0).start()

    def spread(k):
        t = y * half + k

        @pl.when(jnp.logical_not(is_root))
        def _():
            copy_x3(t, 0).wait_recv()

            @pl.when(same_core)
            def _():
                copy_x3(t, 1).start()
                copy_x3(t, 0).start()

    def spread_far(k):
        t = other * half + k
        copy_x3(t, 0).wait_recv()

        @pl.when(same_core)
        def _():
            copy_x3(t, 0).start()

    for k in range(half):
        chain(k)
    def copy_p(t, down):
        to_s = lax.rem(s + n_seq - 2, n_seq) if down else lax.rem(s + 2, n_seq)
        return remote(psend.at[t], precv.at[t], s_p.at[t], r_p.at[t], to_s, h)

    bias = b[:, my_cols(y)]
    out_row = w2[:, my_cols(y)]
    lanes = lax.broadcasted_iota(jnp.int32, (block, 128), 1)
    fsend[...] = jnp.zeros_like(fsend)

    lag = 3

    def reduce_step(tick):
        for down in (True, False):
            first = planes - 1 if down else 0
            last = planes - 1 - first
            k = tick - lag * (planes - 1 - z if down else z)
            t = k if down else half + k

            @pl.when((k >= 0) & (k < half))
            def _():
                psend[t] = jnp.dot(xall[t], wall[...], preferred_element_type=jnp.float32)

                @pl.when(z != first)
                def _():
                    copy_p(t, down).wait_recv()
                    psend[t] = psend[t] + precv[t]

                @pl.when(z != last)
                def _():
                    copy_p(t, down).start()

                @pl.when(z == last)
                def _():
                    act = jnp.maximum(psend[t] + bias, 0.0) * out_row
                    total = jnp.sum(act, axis=1, keepdims=True)
                    here = pl.ds(pl.multiple_of((k % 2) * block, block), block)
                    fsend[here, :] = fsend[here, :] + jnp.where(lanes == t // 2, total, 0.0)

    for k in range(half):
        spread(k)
    for k in range(half):
        spread_far(k)
        if k == 0:
            for i in range(2):
                copy_w(i).wait_recv()
        reduce_step(k)
    for k in range(half, half + lag * (planes - 1)):
        reduce_step(k)

    is_end = (z == 0) | (z == planes - 1)
    slots = 4 * n_head
    me = s * n_head + h
    n_dev = n_seq * n_head
    slot = jnp.where(z == 0, 0, 1) * (2 * n_head) + y * n_head + h

    def copy_f(d):
        to = lax.rem(me + d, n_dev)
        return remote(
            frecv.at[slot], frecv.at[slot], s_f.at[d], r_f.at[slot], to // n_head, lax.rem(to, n_head)
        )

    @pl.when(is_end)
    def _():
        frecv[slot] = jnp.transpose(fsend[...])[: frecv.shape[1], :]
        for d in range(1, n_dev):
            copy_f(d).start()

    logit = jnp.zeros(frecv.shape[1:], jnp.float32)
    for i in range(slots):

        @pl.when(jnp.logical_not(is_end & (slot == i)))
        def _():
            remote(frecv.at[i], frecv.at[i], s_f.at[0], r_f.at[i], across, h).wait_recv()

        logit = logit + frecv[i]

    live = valid[...] == 1
    reward[...] = jnp.where(live, logit, 0.0)
    low = jnp.min(jnp.where(live, logit, 1e30), axis=1, keepdims=True)
    square = (traces, traces)
    eye = lax.broadcasted_iota(jnp.int32, square, 0) == lax.broadcasted_iota(jnp.int32, square, 1)
    score[...] = jnp.sum(jnp.where(eye, low, 0.0), axis=0)
    ids = lax.broadcasted_iota(jnp.int32, (traces, pairs.shape[1]), 0)
    winner = jnp.sum(jnp.where(pairs[0:1, :] == ids, low, 0.0), axis=0)
    loser = jnp.sum(jnp.where(pairs[1:2, :] == ids, low, 0.0), axis=0)
    margin[...] = winner - loser

    for i in range(2):
        copy_w(i).wait_send()
    for k in range(half):
        copy_x1(k).wait_send()

        @pl.when(jnp.logical_not(is_root))
        def _():
            copy_down(k).wait_send()

        for t, near in ((y * half + k, True), (other * half + k, False)):

            @pl.when(same_core)
            def _():
                copy_x3(t, 0).wait_send()
                if near:
                    copy_x3(t, 1).wait_send()

        @pl.when(is_root)
        def _():
            copy_x3(y * half + k, 2).wait_send()

        @pl.when(z != 0)
        def _():
            copy_p(k, True).wait_send()

        @pl.when(z != planes - 1)
        def _():
            copy_p(half + k, False).wait_send()

    @pl.when(is_end)
    def _():
        for d in range(1, n_dev):
            copy_f(d).wait_send()


def fused(n_seq, n_head, hidden_states, boundary, valid, pairs, w_first, b_first, w_second):
    traces, toks, feats = hidden_states.shape
    steps = boundary.shape[1]
    depth, width = w_first.shape
    half, block, cols = traces, steps // 2, width // 2
    bf16, f32 = jnp.bfloat16, jnp.float32
    dma = pltpu.SemaphoreType.DMA
    vmem = pl.BlockSpec(memory_space=pltpu.VMEM)
    hbm = pl.BlockSpec(memory_space=pl.ANY)
    return pl.pallas_call(
        functools.partial(kernel, n_seq, n_head),
        out_shape=(
            jax.ShapeDtypeStruct((traces, steps), f32),
            jax.ShapeDtypeStruct((traces,), f32),
            jax.ShapeDtypeStruct((pairs.shape[0],), f32),
        ),
        in_specs=[hbm] + [vmem] * 3 + [hbm] + [vmem] * 2,
        out_specs=(vmem,) * 3,
        scratch_shapes=[
            pltpu.VMEM((traces, toks, feats), bf16),
            pltpu.VMEM((depth, width), bf16),
            dma, dma,
            pltpu.VMEM((half, block, feats), bf16),
            pltpu.VMEM((half, block, feats), bf16),
            pltpu.VMEM((half, block, feats), bf16),
            pltpu.VMEM((half, block, feats), bf16),
            pltpu.VMEM((half, block, feats), bf16),
            pltpu.VMEM((2 * half, block, feats), bf16),
            pltpu.VMEM((depth, cols), bf16),
            pltpu.VMEM((2 * depth, cols), bf16),
            pltpu.VMEM((2 * half, block, cols), f32),
            pltpu.VMEM((2 * half, block, cols), f32),
            pltpu.VMEM((steps, 128), f32),
            pltpu.VMEM((4 * n_head, traces, steps), f32),
            dma((half,)), dma((half,)),
            dma((2,)), dma((2,)),
            dma((half,)), dma((half,)), dma((half,)),
            dma((2 * half, 3)), dma((2 * half,)),
            dma((2 * half,)), dma((2 * half,)),
            dma((n_seq * n_head,)), dma((4 * n_head,)),
        ],
        compiler_params=pltpu.CompilerParams(collective_id=0, has_side_effects=True),
    )(
        hidden_states, boundary, valid, pairs.T, w_first,
        b_first.reshape(1, width), w_second.reshape(1, width),
    )


def solution(mesh):
    n_seq, n_head = mesh.shape["seq"], mesh.shape["head"]
    paired = n_seq == 2 * n_head and n_head % 4 == 0
    body = functools.partial(fused, n_seq, n_head) if paired else per_device
    placed = (P(None, "seq", "head"), P(), P(), P(), P("seq", "head"), P("head"), P("head"))
    return jax.shard_map(
        body, mesh=mesh, in_specs=placed, out_specs=(P(), P(), P()), check_vma=False
    )
```

```python
import functools

import jax
import jax.numpy as jnp
from jax import lax
from jax.experimental import pallas as pl
from jax.experimental.pallas import tpu as pltpu
from jax.sharding import PartitionSpec as P

MESH = pl.DeviceIdType.MESH


def score_rows(rows, w_first, b_first, w_second):
    pre = jnp.dot(
        rows, lax.all_gather(w_first, "seq", axis=0, tiled=True), preferred_element_type=jnp.float32
    )
    return jnp.sum(jnp.maximum(pre + b_first, 0.0) * w_second, axis=-1)


def per_device(hidden_states, boundary, valid, pairs, w_first, b_first, w_second):
    traces, tok_dev, quarter = hidden_states.shape
    offset = lax.axis_index("seq") * tok_dev
    positions = offset + jnp.arange(tok_dev, dtype=jnp.int32)
    hits = boundary[:, :, None] == positions[None, None, :]
    whole = lax.all_gather(hidden_states, "head", axis=2, tiled=True)
    token_logit = score_rows(
        whole.reshape(traces * tok_dev, whole.shape[2]), w_first, b_first, w_second
    )
    token_logit = token_logit.reshape(traces, tok_dev)
    partial_logit = jnp.sum(jnp.where(hits, token_logit[:, None, :], 0.0), axis=2)
    logit = lax.psum(partial_logit, ("seq", "head"))
    live = valid == 1
    step_reward = jnp.where(live, logit, jnp.float32(0.0))
    trace_score = jnp.min(jnp.where(live, logit, jnp.float32(1e30)), axis=1)
    trace_ids = jnp.arange(traces, dtype=jnp.int32)[None, :]
    winner = jnp.sum(jnp.where(pairs[:, 0:1] == trace_ids, trace_score[None, :], 0.0), axis=1)
    loser = jnp.sum(jnp.where(pairs[:, 1:2] == trace_ids, trace_score[None, :], 0.0), axis=1)
    return (step_reward, trace_score, winner - loser)


def kernel(
    n_seq, n_head, hid_hbm, bnd, valid, pairs, w_hbm, b, w2, reward, score, margin,
    hid, w, s_hid, s_win,
    xout, xin, xacc, xup, xdn, xall, wown, wall, psend, precv, fsend, frecv,
    s_x1, r_x1, s_w, r_w, s_x2, r_up, r_dn, s_x3, r_x3, s_p, r_p, s_f, r_f,
):
    fetch_hid = pltpu.make_async_copy(hid_hbm, hid, s_hid)
    fetch_w = pltpu.make_async_copy(w_hbm, w, s_win)
    fetch_hid.start()
    fetch_w.start()
    traces, toks, _ = hid.shape
    half = traces
    block = bnd.shape[1] // 2
    planes = n_seq // 2
    depth = w.shape[0]
    cols = w.shape[1] // 2
    s = lax.axis_index("seq")
    h = lax.axis_index("head")
    z = s // 2
    y = s % 2
    other = 1 - y

    def remote(src, dst, send, recv, to_s, to_h):
        return pltpu.make_async_remote_copy(
            src_ref=src, dst_ref=dst, send_sem=send, recv_sem=recv,
            device_id=(to_s, to_h), device_id_type=MESH,
        )

    across = s + 1 - 2 * y
    h_core = h + 1 - 2 * (h % 2)
    h_x = lax.rem(h + 2, n_head)

    barrier = pltpu.get_barrier_semaphore()

    def greet(to_s, to_h):
        pl.semaphore_signal(barrier, inc=1, device_id=(to_s, to_h), device_id_type=MESH)

    greet(across, h)
    greet(s, h_core)
    greet(s, h_x)

    @pl.when(z > 0)
    def _():
        greet(s - 2, h)

    @pl.when(z < planes - 1)
    def _():
        greet(s + 2, h)

    def pick(t):
        pos = lax.broadcasted_iota(jnp.int32, (toks, bnd.shape[1]), 0) + s * toks
        hot = jnp.where(bnd[pl.ds(t, 1), :] == pos, 1.0, 0.0).astype(jnp.bfloat16)
        got = lax.dot_general(
            hot, hid[t], (((0,), (0,)), ((), ())), preferred_element_type=jnp.float32
        )
        return got.astype(jnp.bfloat16)

    def copy_x1(k):
        return remote(xout.at[k], xin.at[k], s_x1.at[k], r_x1.at[k], across, h)

    def my_cols(which):
        return pl.ds(pl.multiple_of(which * cols, cols), cols)

    part = depth // 2

    def copy_w(i):
        rows = pl.ds(pl.multiple_of(y * depth + i * part, part), part)
        return remote(wown.at[pl.ds(i * part, part)], wall.at[rows], s_w.at[i], r_w.at[i], across, h)

    def pick_half(which, dst):
        for i in range(traces // 2):
            got = pick(which * (traces // 2) + i)
            dst[2 * i] = got[:block]
            dst[2 * i + 1] = got[block:]

    fetch_hid.wait()
    pick_half(other, xout)
    pl.semaphore_wait(
        barrier, 3 + jnp.where(z > 0, 1, 0) + jnp.where(z < planes - 1, 1, 0)
    )
    for k in range(half):
        copy_x1(k).start()
    fetch_w.wait()
    wown[...] = w[:, my_cols(other)]
    for i in range(2):
        copy_w(i).start()
    wall[pl.ds(pl.multiple_of(y * depth, depth), depth), :] = w[:, my_cols(y)]

    pick_half(y, xacc)

    same_core = (h % 2) == (z % 2)

    def copy_x3(t, way):
        to_s, to_h = ((s, h_core), (across, h), (s, h_x))[way]
        return remote(xall.at[t], xall.at[t], s_x3.at[t, way], r_x3.at[t], to_s, to_h)

    is_root = z == h
    from_up = (z >= h) & (z < planes - 1)
    from_dn = (z <= h) & (z > 0)

    def copy_down(k):
        return remote(xacc.at[k], xup.at[k], s_x2.at[k], r_up.at[k], lax.rem(s + n_seq - 2, n_seq), h)

    def copy_up(k):
        return remote(xacc.at[k], xdn.at[k], s_x2.at[k], r_dn.at[k], lax.rem(s + 2, n_seq), h)

    def chain(k):
        copy_x1(k).wait_recv()
        xacc[k] = xacc[k] + xin[k]

        @pl.when(from_up)
        def _():
            copy_down(k).wait_recv()
            xacc[k] = xacc[k] + xup[k]

        @pl.when(from_dn)
        def _():
            copy_up(k).wait_recv()
            xacc[k] = xacc[k] + xdn[k]

        @pl.when(z > h)
        def _():
            copy_down(k).start()

        @pl.when(z < h)
        def _():
            copy_up(k).start()

        @pl.when(is_root)
        def _():
            t = y * half + k
            xall[t] = xacc[k]
            copy_x3(t, 1).start()
            copy_x3(t, 2).start()
            copy_x3(t, 0).start()

    def spread(k):
        t = y * half + k

        @pl.when(jnp.logical_not(is_root))
        def _():
            copy_x3(t, 0).wait_recv()

            @pl.when(same_core)
            def _():
                copy_x3(t, 1).start()
                copy_x3(t, 0).start()

    def spread_far(k):
        t = other * half + k
        copy_x3(t, 0).wait_recv()

        @pl.when(same_core)
        def _():
            copy_x3(t, 0).start()

    for k in range(half):
        chain(k)
    def copy_p(t, down):
        to_s = lax.rem(s + n_seq - 2, n_seq) if down else lax.rem(s + 2, n_seq)
        return remote(psend.at[t], precv.at[t], s_p.at[t], r_p.at[t], to_s, h)

    bias = b[:, my_cols(y)]
    out_row = w2[:, my_cols(y)]
    lanes = lax.broadcasted_iota(jnp.int32, (block, 128), 1)
    fsend[...] = jnp.zeros_like(fsend)

    lag = 3

    def reduce_step(tick):
        for down in (True, False):
            first = planes - 1 if down else 0
            last = planes - 1 - first
            k = tick - lag * (planes - 1 - z if down else z)
            t = k if down else half + k

            @pl.when((k >= 0) & (k < half))
            def _():
                psend[t] = jnp.dot(xall[t], wall[...], preferred_element_type=jnp.float32)

                @pl.when(z != first)
                def _():
                    copy_p(t, down).wait_recv()
                    psend[t] = psend[t] + precv[t]

                @pl.when(z != last)
                def _():
                    copy_p(t, down).start()

                @pl.when(z == last)
                def _():
                    act = jnp.maximum(psend[t] + bias, 0.0) * out_row
                    total = jnp.sum(act, axis=1, keepdims=True)
                    here = pl.ds(pl.multiple_of((k % 2) * block, block), block)
                    fsend[here, :] = fsend[here, :] + jnp.where(lanes == k // 2, total, 0.0)

    for k in range(half):
        spread(k)
    for k in range(half):
        spread_far(k)
        if k == 0:
            for i in range(2):
                copy_w(i).wait_recv()
        reduce_step(k)
    for k in range(half, half + lag * (planes - 1)):
        reduce_step(k)

    is_end = (z == 0) | (z == planes - 1)
    slots = 4 * n_head
    me = s * n_head + h
    n_dev = n_seq * n_head
    slot = jnp.where(z == 0, 0, 1) * (2 * n_head) + y * n_head + h

    def copy_f(d):
        to = lax.rem(me + d, n_dev)
        return remote(
            frecv.at[slot], frecv.at[slot], s_f.at[d], r_f.at[slot], to // n_head, lax.rem(to, n_head)
        )

    @pl.when(is_end)
    def _():
        frecv[slot] = jnp.transpose(fsend[...])[: frecv.shape[1], :]
        for d in range(1, n_dev):
            copy_f(d).start()

    sums = [jnp.zeros(frecv.shape[1:], jnp.float32) for _ in range(2)]
    for i in range(slots):

        @pl.when(jnp.logical_not(is_end & (slot == i)))
        def _():
            remote(frecv.at[i], frecv.at[i], s_f.at[0], r_f.at[i], across, h).wait_recv()

        side = i // (2 * n_head)
        sums[side] = sums[side] + frecv[i]

    logit = jnp.concatenate(sums, axis=0)

    live = valid[...] == 1
    reward[...] = jnp.where(live, logit, 0.0)
    low = jnp.min(jnp.where(live, logit, 1e30), axis=1, keepdims=True)
    square = (traces, traces)
    eye = lax.broadcasted_iota(jnp.int32, square, 0) == lax.broadcasted_iota(jnp.int32, square, 1)
    score[...] = jnp.sum(jnp.where(eye, low, 0.0), axis=0)
    ids = lax.broadcasted_iota(jnp.int32, (traces, pairs.shape[1]), 0)
    winner = jnp.sum(jnp.where(pairs[0:1, :] == ids, low, 0.0), axis=0)
    loser = jnp.sum(jnp.where(pairs[1:2, :] == ids, low, 0.0), axis=0)
    margin[...] = winner - loser

    for i in range(2):
        copy_w(i).wait_send()
    for k in range(half):
        copy_x1(k).wait_send()

        @pl.when(jnp.logical_not(is_root))
        def _():
            copy_down(k).wait_send()

        for t, near in ((y * half + k, True), (other * half + k, False)):

            @pl.when(same_core)
            def _():
                copy_x3(t, 0).wait_send()
                if near:
                    copy_x3(t, 1).wait_send()

        @pl.when(is_root)
        def _():
            copy_x3(y * half + k, 2).wait_send()

        @pl.when(z != 0)
        def _():
            copy_p(k, True).wait_send()

        @pl.when(z != planes - 1)
        def _():
            copy_p(half + k, False).wait_send()

    @pl.when(is_end)
    def _():
        for d in range(1, n_dev):
            copy_f(d).wait_send()


def fused(n_seq, n_head, hidden_states, boundary, valid, pairs, w_first, b_first, w_second):
    traces, toks, feats = hidden_states.shape
    steps = boundary.shape[1]
    depth, width = w_first.shape
    half, block, cols = traces, steps // 2, width // 2
    bf16, f32 = jnp.bfloat16, jnp.float32
    dma = pltpu.SemaphoreType.DMA
    vmem = pl.BlockSpec(memory_space=pltpu.VMEM)
    hbm = pl.BlockSpec(memory_space=pl.ANY)
    return pl.pallas_call(
        functools.partial(kernel, n_seq, n_head),
        out_shape=(
            jax.ShapeDtypeStruct((traces, steps), f32),
            jax.ShapeDtypeStruct((traces,), f32),
            jax.ShapeDtypeStruct((pairs.shape[0],), f32),
        ),
        in_specs=[hbm] + [vmem] * 3 + [hbm] + [vmem] * 2,
        out_specs=(vmem,) * 3,
        scratch_shapes=[
            pltpu.VMEM((traces, toks, feats), bf16),
            pltpu.VMEM((depth, width), bf16),
            dma, dma,
            pltpu.VMEM((half, block, feats), bf16),
            pltpu.VMEM((half, block, feats), bf16),
            pltpu.VMEM((half, block, feats), bf16),
            pltpu.VMEM((half, block, feats), bf16),
            pltpu.VMEM((half, block, feats), bf16),
            pltpu.VMEM((2 * half, block, feats), bf16),
            pltpu.VMEM((depth, cols), bf16),
            pltpu.VMEM((2 * depth, cols), bf16),
            pltpu.VMEM((2 * half, block, cols), f32),
            pltpu.VMEM((2 * half, block, cols), f32),
            pltpu.VMEM((steps, 128), f32),
            pltpu.VMEM((4 * n_head, traces // 2, steps), f32),
            dma((half,)), dma((half,)),
            dma((2,)), dma((2,)),
            dma((half,)), dma((half,)), dma((half,)),
            dma((2 * half, 3)), dma((2 * half,)),
            dma((2 * half,)), dma((2 * half,)),
            dma((n_seq * n_head,)), dma((4 * n_head,)),
        ],
        compiler_params=pltpu.CompilerParams(collective_id=0, has_side_effects=True),
    )(
        hidden_states, boundary, valid, pairs.T, w_first,
        b_first.reshape(1, width), w_second.reshape(1, width),
    )


def solution(mesh):
    n_seq, n_head = mesh.shape["seq"], mesh.shape["head"]
    paired = n_seq == 2 * n_head and n_head % 4 == 0
    body = functools.partial(fused, n_seq, n_head) if paired else per_device
    placed = (P(None, "seq", "head"), P(), P(), P(), P("seq", "head"), P("head"), P("head"))
    return jax.shard_map(
        body, mesh=mesh, in_specs=placed, out_specs=(P(), P(), P()), check_vma=False
    )
```

```python
import functools

import jax
import jax.numpy as jnp
from jax import lax
from jax.experimental import pallas as pl
from jax.experimental.pallas import tpu as pltpu
from jax.sharding import PartitionSpec as P

MESH = pl.DeviceIdType.MESH


def score_rows(rows, w_first, b_first, w_second):
    pre = jnp.dot(
        rows, lax.all_gather(w_first, "seq", axis=0, tiled=True), preferred_element_type=jnp.float32
    )
    return jnp.sum(jnp.maximum(pre + b_first, 0.0) * w_second, axis=-1)


def per_device(hidden_states, boundary, valid, pairs, w_first, b_first, w_second):
    traces, tok_dev, quarter = hidden_states.shape
    offset = lax.axis_index("seq") * tok_dev
    positions = offset + jnp.arange(tok_dev, dtype=jnp.int32)
    hits = boundary[:, :, None] == positions[None, None, :]
    whole = lax.all_gather(hidden_states, "head", axis=2, tiled=True)
    token_logit = score_rows(
        whole.reshape(traces * tok_dev, whole.shape[2]), w_first, b_first, w_second
    )
    token_logit = token_logit.reshape(traces, tok_dev)
    partial_logit = jnp.sum(jnp.where(hits, token_logit[:, None, :], 0.0), axis=2)
    logit = lax.psum(partial_logit, ("seq", "head"))
    live = valid == 1
    step_reward = jnp.where(live, logit, jnp.float32(0.0))
    trace_score = jnp.min(jnp.where(live, logit, jnp.float32(1e30)), axis=1)
    trace_ids = jnp.arange(traces, dtype=jnp.int32)[None, :]
    winner = jnp.sum(jnp.where(pairs[:, 0:1] == trace_ids, trace_score[None, :], 0.0), axis=1)
    loser = jnp.sum(jnp.where(pairs[:, 1:2] == trace_ids, trace_score[None, :], 0.0), axis=1)
    return (step_reward, trace_score, winner - loser)


def kernel(
    n_seq, n_head, hid_hbm, bnd, valid, pairs, w_hbm, b, w2, reward, score, margin,
    hid, w, s_hid, s_win,
    xout, xin, xacc, xup, xdn, xall, wown, wall, psend, precv, fsend, frecv,
    s_x1, r_x1, s_w, r_w, s_x2, r_up, r_dn, s_x3, r_x3, s_p, r_p, s_f, r_f,
):
    fetch_hid = pltpu.make_async_copy(hid_hbm, hid, s_hid)
    fetch_w = pltpu.make_async_copy(w_hbm, w, s_win)
    fetch_hid.start()
    fetch_w.start()
    traces, toks, _ = hid.shape
    half = traces
    block = bnd.shape[1] // 2
    planes = n_seq // 2
    depth = w.shape[0]
    cols = w.shape[1] // 2
    s = lax.axis_index("seq")
    h = lax.axis_index("head")
    z = s // 2
    y = s % 2
    other = 1 - y

    def remote(src, dst, send, recv, to_s, to_h):
        return pltpu.make_async_remote_copy(
            src_ref=src, dst_ref=dst, send_sem=send, recv_sem=recv,
            device_id=(to_s, to_h), device_id_type=MESH,
        )

    across = s + 1 - 2 * y
    h_core = h + 1 - 2 * (h % 2)
    h_x = lax.rem(h + 2, n_head)

    barrier = pltpu.get_barrier_semaphore()

    def greet(to_s, to_h):
        pl.semaphore_signal(barrier, inc=1, device_id=(to_s, to_h), device_id_type=MESH)

    greet(across, h)
    greet(s, h_core)
    greet(s, h_x)

    @pl.when(z > 0)
    def _():
        greet(s - 2, h)

    @pl.when(z < planes - 1)
    def _():
        greet(s + 2, h)

    def pick(t):
        pos = lax.broadcasted_iota(jnp.int32, (toks, bnd.shape[1]), 0) + s * toks
        hot = jnp.where(bnd[pl.ds(t, 1), :] == pos, 1.0, 0.0).astype(jnp.bfloat16)
        got = lax.dot_general(
            hot, hid[t], (((0,), (0,)), ((), ())), preferred_element_type=jnp.float32
        )
        return got.astype(jnp.bfloat16)

    def copy_x1(k):
        return remote(xout.at[k], xin.at[k], s_x1.at[k], r_x1.at[k], across, h)

    def my_cols(which):
        return pl.ds(pl.multiple_of(which * cols, cols), cols)

    part = depth // 2

    def copy_w(i):
        rows = pl.ds(pl.multiple_of(y * depth + i * part, part), part)
        return remote(wown.at[pl.ds(i * part, part)], wall.at[rows], s_w.at[i], r_w.at[i], across, h)

    def pick_half(which, dst, send):
        for i in range(traces // 2):
            got = pick(which * (traces // 2) + i)
            dst[2 * i] = got[:block]
            dst[2 * i + 1] = got[block:]
            if send:
                copy_x1(2 * i).start()
                copy_x1(2 * i + 1).start()

    fetch_hid.wait()
    pl.semaphore_wait(
        barrier, 3 + jnp.where(z > 0, 1, 0) + jnp.where(z < planes - 1, 1, 0)
    )
    pick_half(other, xout, True)
    fetch_w.wait()
    wown[...] = w[:, my_cols(other)]
    for i in range(2):
        copy_w(i).start()
    wall[pl.ds(pl.multiple_of(y * depth, depth), depth), :] = w[:, my_cols(y)]

    pick_half(y, xacc, False)

    same_core = (h % 2) == (z % 2)

    def copy_x3(t, way):
        to_s, to_h = ((s, h_core), (across, h), (s, h_x))[way]
        return remote(xall.at[t], xall.at[t], s_x3.at[t, way], r_x3.at[t], to_s, to_h)

    is_root = z == h
    from_up = (z >= h) & (z < planes - 1)
    from_dn = (z <= h) & (z > 0)

    def copy_down(k):
        return remote(xacc.at[k], xup.at[k], s_x2.at[k], r_up.at[k], lax.rem(s + n_seq - 2, n_seq), h)

    def copy_up(k):
        return remote(xacc.at[k], xdn.at[k], s_x2.at[k], r_dn.at[k], lax.rem(s + 2, n_seq), h)

    def chain(k):
        copy_x1(k).wait_recv()
        xacc[k] = xacc[k] + xin[k]

        @pl.when(from_up)
        def _():
            copy_down(k).wait_recv()
            xacc[k] = xacc[k] + xup[k]

        @pl.when(from_dn)
        def _():
            copy_up(k).wait_recv()
            xacc[k] = xacc[k] + xdn[k]

        @pl.when(z > h)
        def _():
            copy_down(k).start()

        @pl.when(z < h)
        def _():
            copy_up(k).start()

        @pl.when(is_root)
        def _():
            t = y * half + k
            xall[t] = xacc[k]
            copy_x3(t, 1).start()
            copy_x3(t, 2).start()
            copy_x3(t, 0).start()

    def spread(k):
        t = y * half + k

        @pl.when(jnp.logical_not(is_root))
        def _():
            copy_x3(t, 0).wait_recv()

            @pl.when(same_core)
            def _():
                copy_x3(t, 1).start()
                copy_x3(t, 0).start()

    def spread_far(k):
        t = other * half + k
        copy_x3(t, 0).wait_recv()

        @pl.when(same_core)
        def _():
            copy_x3(t, 0).start()

    for k in range(half):
        chain(k)
    def copy_p(t, down):
        to_s = lax.rem(s + n_seq - 2, n_seq) if down else lax.rem(s + 2, n_seq)
        return remote(psend.at[t], precv.at[t], s_p.at[t], r_p.at[t], to_s, h)

    bias = b[:, my_cols(y)]
    out_row = w2[:, my_cols(y)]
    lanes = lax.broadcasted_iota(jnp.int32, (block, 128), 1)
    fsend[...] = jnp.zeros_like(fsend)

    lag = 3

    def reduce_step(tick):
        for down in (True, False):
            first = planes - 1 if down else 0
            last = planes - 1 - first
            k = tick - lag * (planes - 1 - z if down else z)
            t = k if down else half + k

            @pl.when((k >= 0) & (k < half))
            def _():
                psend[t] = jnp.dot(xall[t], wall[...], preferred_element_type=jnp.float32)

                @pl.when(z != first)
                def _():
                    copy_p(t, down).wait_recv()
                    psend[t] = psend[t] + precv[t]

                @pl.when(z != last)
                def _():
                    copy_p(t, down).start()

                @pl.when(z == last)
                def _():
                    act = jnp.maximum(psend[t] + bias, 0.0) * out_row
                    total = jnp.sum(act, axis=1, keepdims=True)
                    here = pl.ds(pl.multiple_of((k % 2) * block, block), block)
                    fsend[here, :] = fsend[here, :] + jnp.where(lanes == k // 2, total, 0.0)

    for k in range(half):
        spread(k)
    for k in range(half):
        spread_far(k)
        if k == 0:
            for i in range(2):
                copy_w(i).wait_recv()
        reduce_step(k)
    for k in range(half, half + lag * (planes - 1)):
        reduce_step(k)

    is_end = (z == 0) | (z == planes - 1)
    slots = 4 * n_head
    me = s * n_head + h
    n_dev = n_seq * n_head
    slot = jnp.where(z == 0, 0, 1) * (2 * n_head) + y * n_head + h

    def copy_f(d):
        to = lax.rem(me + d, n_dev)
        return remote(
            frecv.at[slot], frecv.at[slot], s_f.at[d], r_f.at[slot], to // n_head, lax.rem(to, n_head)
        )

    @pl.when(is_end)
    def _():
        frecv[slot] = jnp.transpose(fsend[...])[: frecv.shape[1], :]
        for d in range(1, n_dev):
            copy_f(d).start()

    sums = [jnp.zeros(frecv.shape[1:], jnp.float32) for _ in range(2)]
    for i in range(slots):

        @pl.when(jnp.logical_not(is_end & (slot == i)))
        def _():
            remote(frecv.at[i], frecv.at[i], s_f.at[0], r_f.at[i], across, h).wait_recv()

        side = i // (2 * n_head)
        sums[side] = sums[side] + frecv[i]

    logit = jnp.concatenate(sums, axis=0)

    live = valid[...] == 1
    reward[...] = jnp.where(live, logit, 0.0)
    low = jnp.min(jnp.where(live, logit, 1e30), axis=1, keepdims=True)
    square = (traces, traces)
    eye = lax.broadcasted_iota(jnp.int32, square, 0) == lax.broadcasted_iota(jnp.int32, square, 1)
    score[...] = jnp.sum(jnp.where(eye, low, 0.0), axis=0)
    ids = lax.broadcasted_iota(jnp.int32, (traces, pairs.shape[1]), 0)
    winner = jnp.sum(jnp.where(pairs[0:1, :] == ids, low, 0.0), axis=0)
    loser = jnp.sum(jnp.where(pairs[1:2, :] == ids, low, 0.0), axis=0)
    margin[...] = winner - loser

    for i in range(2):
        copy_w(i).wait_send()
    for k in range(half):
        copy_x1(k).wait_send()

        @pl.when(jnp.logical_not(is_root))
        def _():
            copy_down(k).wait_send()

        for t, near in ((y * half + k, True), (other * half + k, False)):

            @pl.when(same_core)
            def _():
                copy_x3(t, 0).wait_send()
                if near:
                    copy_x3(t, 1).wait_send()

        @pl.when(is_root)
        def _():
            copy_x3(y * half + k, 2).wait_send()

        @pl.when(z != 0)
        def _():
            copy_p(k, True).wait_send()

        @pl.when(z != planes - 1)
        def _():
            copy_p(half + k, False).wait_send()

    @pl.when(is_end)
    def _():
        for d in range(1, n_dev):
            copy_f(d).wait_send()


def fused(n_seq, n_head, hidden_states, boundary, valid, pairs, w_first, b_first, w_second):
    traces, toks, feats = hidden_states.shape
    steps = boundary.shape[1]
    depth, width = w_first.shape
    half, block, cols = traces, steps // 2, width // 2
    bf16, f32 = jnp.bfloat16, jnp.float32
    dma = pltpu.SemaphoreType.DMA
    vmem = pl.BlockSpec(memory_space=pltpu.VMEM)
    hbm = pl.BlockSpec(memory_space=pl.ANY)
    return pl.pallas_call(
        functools.partial(kernel, n_seq, n_head),
        out_shape=(
            jax.ShapeDtypeStruct((traces, steps), f32),
            jax.ShapeDtypeStruct((traces,), f32),
            jax.ShapeDtypeStruct((pairs.shape[0],), f32),
        ),
        in_specs=[hbm] + [vmem] * 3 + [hbm] + [vmem] * 2,
        out_specs=(vmem,) * 3,
        scratch_shapes=[
            pltpu.VMEM((traces, toks, feats), bf16),
            pltpu.VMEM((depth, width), bf16),
            dma, dma,
            pltpu.VMEM((half, block, feats), bf16),
            pltpu.VMEM((half, block, feats), bf16),
            pltpu.VMEM((half, block, feats), bf16),
            pltpu.VMEM((half, block, feats), bf16),
            pltpu.VMEM((half, block, feats), bf16),
            pltpu.VMEM((2 * half, block, feats), bf16),
            pltpu.VMEM((depth, cols), bf16),
            pltpu.VMEM((2 * depth, cols), bf16),
            pltpu.VMEM((2 * half, block, cols), f32),
            pltpu.VMEM((2 * half, block, cols), f32),
            pltpu.VMEM((steps, 128), f32),
            pltpu.VMEM((4 * n_head, traces // 2, steps), f32),
            dma((half,)), dma((half,)),
            dma((2,)), dma((2,)),
            dma((half,)), dma((half,)), dma((half,)),
            dma((2 * half, 3)), dma((2 * half,)),
            dma((2 * half,)), dma((2 * half,)),
            dma((n_seq * n_head,)), dma((4 * n_head,)),
        ],
        compiler_params=pltpu.CompilerParams(collective_id=0, has_side_effects=True),
    )(
        hidden_states, boundary, valid, pairs.T, w_first,
        b_first.reshape(1, width), w_second.reshape(1, width),
    )


def solution(mesh):
    n_seq, n_head = mesh.shape["seq"], mesh.shape["head"]
    paired = n_seq == 2 * n_head and n_head % 4 == 0
    body = functools.partial(fused, n_seq, n_head) if paired else per_device
    placed = (P(None, "seq", "head"), P(), P(), P(), P("seq", "head"), P("head"), P("head"))
    return jax.shard_map(
        body, mesh=mesh, in_specs=placed, out_specs=(P(), P(), P()), check_vma=False
    )
```
